32 devices in a mesh: dp: 4 (over x, core), space: 8 (over z, y).
Axes of the slice: x: 2, y: 2, z: 4, core: 2. Of those that a mesh axis runs over, the one named last changes fastest.
Arguments:
- section_three: bfloat16 [4, 64, 128, 512], P('dp', 'space'), parts along dimension 0, may hold values from -6 to 6
- section_four: bfloat16 [4, 32, 64, 1024], P('dp', 'space'), parts along dimension 0, may hold values from -6 to 6
- section_five: bfloat16 [4, 16, 32, 2048], P('dp', 'space'), parts along dimension 0, may hold values from -6 to 6
- lateral_three: bfloat16 [512, 256], P('space'), may hold values from -0.25 to 0.25
- lateral_four: bfloat16 [1024, 256], P('space'), may hold values from -0.1875 to 0.1875
- lateral_five: bfloat16 [2048, 256], P('space'), may hold values from -0.125 to 0.125
- lateral_bias_three: float32 [256], replicated, may hold values from -3 to 3
- lateral_bias_four: float32 [256], replicated, may hold values from -3 to 3
- lateral_bias_five: float32 [256], replicated, may hold values from -3 to 3
- output_three: bfloat16 [3, 3, 256, 256], P(None, None, 'space'), may hold values from -0.125 to 0.125
- output_four: bfloat16 [3, 3, 256, 256], P(None, None, 'space'), may hold values from -0.125 to 0.125
- output_five: bfloat16 [3, 3, 256, 256], P(None, None, 'space'), may hold values from -0.125 to 0.125
- output_bias_three: float32 [256], replicated, may hold values from -3 to 3
- output_bias_four: float32 [256], replicated, may hold values from -3 to 3
- output_bias_five: float32 [256], replicated, may hold values from -3 to 3
Outputs:
- level_three: bfloat16 [4, 64, 128, 256], P('dp', 'space'), parts along dimension 0
- level_four: bfloat16 [4, 32, 64, 256], P('dp', 'space'), parts along dimension 0
- level_five: bfloat16 [4, 16, 32, 256], P('dp'), parts along dimension 0
- level_six: bfloat16 [4, 8, 16, 256], P('dp'), parts along dimension 0
The draws below stay inside these ranges and needn't reach their ends.
There are 4 independent parts, one for each index of `dp`. The reference program is written for one: setup_inputs(seed, part) draws one part's arguments, and reference() takes and returns one part's arrays. A program takes and returns all parts, laid end to end along the dimension named above; an argument that names none is the same for every part. Nothing has to cross between parts.
All inputs are finite; a program needn't handle non-finite values.
Results may differ from the reference program's by a relative error of at most 0.0095.
Values may be sent and summed in bfloat16 or wider, within the bound.
A program may use at most 64 MiB of HBM per device.

```python
import jax
import jax.numpy as jnp

C3 = 512
C4 = 1024
C5 = 2048
FD = 256
IMG = 1
W5 = 32
H5 = 16
H4 = 32
H3 = 64
W4 = 64
W3 = 128


def levels(own_key, shape, shards, low, high):
    gain, own = 1.0, jax.random.fold_in(own_key, 6)
    for dim, shards_of in shards:
        draws = jnp.exp(jax.random.uniform(jax.random.fold_in(own, dim), (shards_of,), jnp.float32, low / len(shards), high / len(shards)))
        gain = gain * jnp.repeat(draws, shape[dim] // shards_of).reshape([-1 if axis == dim else 1 for axis in range(len(shape))])
    return gain


def gaussian(key, shape, width, reach, split=(), dtype=jnp.bfloat16):
    values = width * jax.random.normal(key, shape, jnp.float32)
    if split:
        values = values * levels(key, shape, split, -0.22, 0.18)
    return jnp.clip(values, -reach, reach).astype(dtype)


def setup_inputs(seed: int = 0, part: int = 0) -> dict:
    key_of = jax.random.split(jax.random.key(seed), 16)
    part_keys = jax.random.split(jax.random.fold_in(key_of[15], part), 16)
    section_three = gaussian(part_keys[0], (IMG, H3, W3, C3), 1.0, 6.0, ((1, 8),))
    section_four = gaussian(part_keys[1], (IMG, H4, W4, C4), 1.0, 6.0, ((1, 8),))
    section_five = gaussian(part_keys[2], (IMG, H5, W5, C5), 1.0, 6.0, ((1, 8),))
    lateral_three = gaussian(key_of[3], (C3, FD), C3 ** -0.5, 0.25, ((0, 8),))
    lateral_four = gaussian(key_of[4], (C4, FD), C4 ** -0.5, 0.1875, ((0, 8),))
    lateral_five = gaussian(key_of[5], (C5, FD), C5 ** -0.5, 0.125, ((0, 8),))
    lateral_bias_three = gaussian(key_of[6], (FD,), 0.5, 3.0, (), jnp.float32)
    lateral_bias_four = gaussian(key_of[7], (FD,), 0.5, 3.0, (), jnp.float32)
    lateral_bias_five = gaussian(key_of[8], (FD,), 0.5, 3.0, (), jnp.float32)
    output_three = gaussian(key_of[9], (3, 3, FD, FD), (9 * FD) ** -0.5, 0.125, ((2, 8),))
    output_four = gaussian(key_of[10], (3, 3, FD, FD), (9 * FD) ** -0.5, 0.125, ((2, 8),))
    output_five = gaussian(key_of[11], (3, 3, FD, FD), (9 * FD) ** -0.5, 0.125, ((2, 8),))
    output_bias_three = gaussian(key_of[12], (FD,), 0.5, 3.0, (), jnp.float32)
    output_bias_four = gaussian(key_of[13], (FD,), 0.5, 3.0, (), jnp.float32)
    output_bias_five = gaussian(key_of[14], (FD,), 0.5, 3.0, (), jnp.float32)
    return dict(section_three=section_three, section_four=section_four, section_five=section_five, lateral_three=lateral_three, lateral_four=lateral_four, lateral_five=lateral_five, lateral_bias_three=lateral_bias_three, lateral_bias_four=lateral_bias_four, lateral_bias_five=lateral_bias_five, output_three=output_three, output_four=output_four, output_five=output_five, output_bias_three=output_bias_three, output_bias_four=output_bias_four, output_bias_five=output_bias_five)


def lateral(features, weight, offset):
    images, rows, columns, channels = features.shape
    summed = jnp.dot(features.reshape(-1, channels), weight, preferred_element_type=jnp.float32) + offset
    return summed.reshape(images, rows, columns, -1)


def enlarge(coarse):
    return jnp.repeat(jnp.repeat(coarse, 2, axis=1), 2, axis=2)


def conv_rows(padded, weight, offset):
    images, rows_in, columns, channels = padded.shape
    height = rows_in - 2
    framed = jnp.pad(padded, ((0, 0), (0, 0), (1, 1), (0, 0)))
    summed = jnp.zeros((images * height * columns, weight.shape[3]), jnp.float32)
    for row_off in range(3):
        for col_off in range(3):
            window = framed[:, row_off:row_off + height, col_off:col_off + columns, :].reshape(-1, channels)
            summed = summed + jnp.dot(window, weight[row_off, col_off], preferred_element_type=jnp.float32)
    return (summed + offset).reshape(images, height, columns, -1).astype(jnp.bfloat16)


def pad_rows(field):
    return jnp.pad(field, ((0, 0), (1, 1), (0, 0), (0, 0)))


def reference(section_three, section_four, section_five, lateral_three, lateral_four, lateral_five, lateral_bias_three, lateral_bias_four, lateral_bias_five, output_three, output_four, output_five, output_bias_three, output_bias_four, output_bias_five):
    merged_five = lateral(section_five, lateral_five, lateral_bias_five).astype(jnp.bfloat16)
    merged_four = (lateral(section_four, lateral_four, lateral_bias_four) + enlarge(merged_five).astype(jnp.float32)).astype(jnp.bfloat16)
    merged_three = (lateral(section_three, lateral_three, lateral_bias_three) + enlarge(merged_four).astype(jnp.float32)).astype(jnp.bfloat16)
    level_three = conv_rows(pad_rows(merged_three), output_three, output_bias_three)
    level_four = conv_rows(pad_rows(merged_four), output_four, output_bias_four)
    level_five = conv_rows(pad_rows(merged_five), output_five, output_bias_five)
    level_six = level_five[:, ::2, ::2, :]
    return (level_three, level_four, level_five, level_six)
```

```python
import functools

import jax
import jax.numpy as jnp
from jax import lax
from jax.experimental import pallas as pl
from jax.experimental.pallas import tpu as pltpu
from jax.sharding import PartitionSpec as P

F32, BF16 = jnp.float32, jnp.bfloat16


def ring_place(s, n):
    return s // 2 + (s % 2) * (n - 1 - 2 * (s // 2))


def ring_owner(place, n):
    r = (place + 2 * n) % n
    back = r // (n // 2)
    return (1 - back) * (2 * r) + back * (2 * (n - 1 - r) + 1)


def spread(coarse):
    pixels = coarse.shape[0]
    fine = lax.broadcasted_iota(jnp.int32, (2 * pixels, pixels), 0) // 2
    pick = (fine == lax.broadcasted_iota(jnp.int32, (2 * pixels, pixels), 1)).astype(BF16)
    return jnp.dot(pick, coarse, preferred_element_type=F32)


def conv_tile(frame, weight, bias, start, pixels, width):
    rows = jnp.concatenate(
        [frame[pl.ds(pl.multiple_of(start + a * width, 16), pixels), :] for a in range(3)], axis=1
    )
    depth = weight.shape[2]
    part = [
        jnp.dot(
            rows,
            weight[:, c].reshape(3 * depth, weight.shape[3]),
            preferred_element_type=F32,
        )
        for c in range(3)
    ]
    column = lax.broadcasted_iota(jnp.int32, (pixels, 1), 0) % width
    left = jnp.where(column == 0, 0.0, pltpu.roll(part[0], 1, 0))
    right = jnp.where(column == width - 1, 0.0, pltpu.roll(part[2], pixels - 1, 0))
    return part[1] + left + right + bias[...]


def kernel(
    n, dims,
    s3, s4, s5, l3, l4, l5, lb3, lb4, lb5, o3, o4, o5, ob3, ob4, ob5,
    y3, y4, y5, y6,
    v3, v4, v5, w_l5, w_l4, w_l3, w_o3, w_o5, w_o4,
    m3, m4, m5, r3, r4, r5, r6,
    ring_send, ring_recv, core_send, core_recv, halo_send, halo_recv, local_sem,
):
    (rows3, wid3), (rows4, wid4), (rows5, wid5) = dims
    dp, s = lax.axis_index("dp"), lax.axis_index("space")
    core = dp % 2
    partner = (dp + 1 - 2 * core, s)
    place = ring_place(s, n)
    sign = 1 - 2 * core
    hops = (n // 2, n - 1 - n // 2)
    turn = (sign, -sign)
    target = [(dp, ring_owner(place + turn[k], n)) for k in range(2)]
    above, below = (dp, (s + n - 1) % n), (dp, (s + 1) % n)

    full = (w_l5, w_l4, w_l3, w_o3, w_o5, w_o4, m5)
    mine = (l5, l4, l3, o3, o5, o4)
    half = w_l5.shape[1] // 2
    MAP = 6

    def chunk(a, owner, side):
        cols = pl.ds(pl.multiple_of(side * half, half), half)
        if a == MAP:
            size = rows5 * wid5
            return m5.at[pl.ds(pl.multiple_of(wid5 + owner * size, 16), size), :]
        if a < 3:
            size = mine[a].shape[0]
            return full[a].at[pl.ds(pl.multiple_of(owner * size, size), size), cols]
        size = mine[a].shape[2]
        return full[a].at[:, :, pl.ds(pl.multiple_of(owner * size, size), size), cols]

    def own_part(a):
        cols = pl.ds(pl.multiple_of(core * half, half), half)
        return mine[a].at[:, cols] if a < 3 else mine[a].at[:, :, :, cols]

    def own_whole(a):
        if a < 3:
            size = mine[a].shape[0]
            return full[a].at[pl.ds(pl.multiple_of(s * size, size), size), :]
        size = mine[a].shape[2]
        return full[a].at[:, :, pl.ds(pl.multiple_of(s * size, size), size), :]

    local = [pltpu.make_async_copy(mine[a], own_whole(a), local_sem.at[a]) for a in range(6)]
    features = [
        pltpu.make_async_copy(src, dst, local_sem.at[6 + k])
        for k, (src, dst) in enumerate(((s5, v5), (s4, v4), (s3, v3)))
    ]
    for copy in features + local:
        copy.start()

    barrier = pltpu.get_barrier_semaphore()
    for device in (target[0], target[1], partner, above, below):
        pl.semaphore_signal(
            barrier, inc=1, device_id=device, device_id_type=pl.DeviceIdType.MESH
        )
    pl.semaphore_wait(barrier, 5)

    def remote(src, dst, send, recv, device):
        return pltpu.make_async_remote_copy(
            src_ref=src, dst_ref=dst, send_sem=send, recv_sem=recv,
            device_id=device, device_id_type=pl.DeviceIdType.MESH,
        )

    sent = []

    def push(a, k, step):
        if step > hops[k]:
            return
        owner = ring_owner(place - turn[k] * (step - 1), n)
        dst = chunk(a, owner, core)
        src = own_part(a) if step == 1 and a != MAP else dst
        copy = remote(src, dst, ring_send.at[a, k, step - 1], ring_recv.at[a, k, step - 1], target[k])
        copy.start()
        sent.append(copy)

    def cross(a, k, step, side, turns):
        owner = ring_owner(place - turns[k] * step, n)
        spot = chunk(a, owner, side)
        j = k * hops[0] + step - 1
        return remote(spot, spot, core_send.at[a, j], core_recv.at[a, j], partner)

    def pull(a, step):
        for k in range(2):
            if step > hops[k]:
                continue
            owner = ring_owner(place - turn[k] * step, n)
            spot = chunk(a, owner, core)
            remote(
                spot, spot, ring_send.at[a, k, step - 1], ring_recv.at[a, k, step - 1], target[k]
            ).wait_recv()
            push(a, k, step + 1)
            if a != MAP:
                copy = cross(a, k, step, core, turn)
                copy.start()
                sent.append(copy)

    def settle(a):
        for k in range(2):
            for step in range(1, hops[k] + 1):
                cross(a, k, step, 1 - core, (turn[1], turn[0])).wait_recv()
        local[a].wait()

    for a in (0, 1, 2):
        push(a, 0, 1)
        push(a, 1, 1)
    waiting = [3, 4, 5]
    for step in range(1, hops[0] + 1):
        if waiting:
            a = waiting.pop(0)
            push(a, 0, 1)
            push(a, 1, 1)
        for a in (0, 1, 2):
            pull(a, step)
    while waiting:
        a = waiting.pop(0)
        push(a, 0, 1)
        push(a, 1, 1)
    for a in (3, 4, 5):
        pull(a, 1)

    settle(0)
    features[0].wait()
    zero5 = jnp.zeros((wid5, m5.shape[1]), BF16)
    m5[pl.ds(0, wid5), :] = zero5
    m5[pl.ds(m5.shape[0] - wid5, wid5), :] = zero5
    here = pl.multiple_of(wid5 + s * (rows5 * wid5), 16)
    m5[pl.ds(here, rows5 * wid5), :] = (
        jnp.dot(v5[...], w_l5[...], preferred_element_type=F32) + lb5[...]
    ).astype(BF16)
    settle(1)
    features[1].wait()
    for r in range(rows5):
        up = spread(m5[pl.ds(pl.multiple_of(here + r * wid5, 16), wid5), :])
        base = 2 * r * wid4
        lat = jnp.dot(v4[base : base + 2 * wid4, :], w_l4[...], preferred_element_type=F32)
        m4[wid4 + base : wid4 + base + 2 * wid4, :] = (
            lat + lb4[...] + jnp.concatenate([up, up], axis=0)
        ).astype(BF16)
    push(MAP, 0, 1)
    push(MAP, 1, 1)
    settle(2)
    features[2].wait()

    def coarse_row(r, carry):
        up = spread(m4[pl.ds(pl.multiple_of(wid4 + r * wid4, 16), wid4), :])
        base = pl.multiple_of(2 * r * wid3, 16)
        lat = jnp.dot(v3[pl.ds(base, 2 * wid3), :], w_l3[...], preferred_element_type=F32)
        m3[pl.ds(pl.multiple_of(wid3 + base, 16), 2 * wid3), :] = (
            lat + lb3[...] + jnp.concatenate([up, up], axis=0)
        ).astype(BF16)
        return carry

    lax.fori_loop(0, rows4, coarse_row, 0)

    halos = []
    for k, (frame, rows, wid) in enumerate(((m4, rows4, wid4), (m3, rows3, wid3))):
        first, last = frame.at[pl.ds(wid, wid), :], frame.at[pl.ds(rows * wid, wid), :]
        top, bottom = frame.at[pl.ds(0, wid), :], frame.at[pl.ds((rows + 1) * wid, wid), :]
        halos.append((
            remote(last, top, halo_send.at[2 * k], halo_recv.at[2 * k], below),
            remote(first, bottom, halo_send.at[2 * k + 1], halo_recv.at[2 * k + 1], above),
        ))
    for step in range(2, hops[0]):
        for a in (3, 4, 5):
            pull(a, step)
        if step == 2:
            for pair in halos:
                for copy in pair:
                    copy.start()
        pull(MAP, step - 1)
    pull(3, hops[0])

    for pair, frame, rows, wid in zip(halos, (m4, m3), (rows4, rows3), (wid4, wid3)):
        for copy in pair:
            copy.wait_recv()
            sent.append(copy)
        zero = jnp.zeros((wid, frame.shape[1]), BF16)

        @pl.when(s == 0)
        def _():
            frame[pl.ds(0, wid), :] = zero

        @pl.when(s == n - 1)
        def _():
            frame[pl.ds((rows + 1) * wid, wid), :] = zero

    settle(3)

    def conv(frame, weight, bias, out, rows, wid, tall):
        def tile(i, carry):
            start = pl.multiple_of(i * (tall * wid), 16)
            out[pl.ds(start, tall * wid), :] = conv_tile(
                frame, weight, bias, start, tall * wid, wid
            ).astype(BF16)
            return carry

        lax.fori_loop(0, rows // tall, tile, 0)

    conv(m3, w_o3, ob3, r3, rows3, wid3, 2)
    out3 = pltpu.make_async_copy(r3, y3, local_sem.at[9])
    out3.start()

    pull(4, hops[0])
    pull(MAP, hops[0] - 1)
    pull(MAP, hops[0])
    pull(5, hops[0])
    settle(4)
    tall5 = 8
    conv(m5, w_o5, ob5, r5, n * rows5, wid5, tall5)
    out5 = pltpu.make_async_copy(r5, y5, local_sem.at[10])
    out5.start()
    take = lax.broadcasted_iota(jnp.int32, (wid5 // 2, wid5), 0) * 2
    pick = (take == lax.broadcasted_iota(jnp.int32, (wid5 // 2, wid5), 1)).astype(BF16)

    def even_row(i, carry):
        row = r5[pl.ds(pl.multiple_of(2 * i * wid5, 16), wid5), :]
        r6[pl.ds(pl.multiple_of(i * (wid5 // 2), 16), wid5 // 2), :] = jnp.dot(
            pick, row, preferred_element_type=F32
        ).astype(BF16)
        return carry

    lax.fori_loop(0, n * rows5 // 2, even_row, 0)
    out6 = pltpu.make_async_copy(r6, y6, local_sem.at[11])
    out6.start()

    settle(5)
    conv(m4, w_o4, ob4, r4, rows4, wid4, rows4)
    out4 = pltpu.make_async_copy(r4, y4, local_sem.at[12])
    out4.start()

    for copy in sent:
        copy.wait_send()
    for copy in (out3, out5, out6, out4):
        copy.wait()


def on_device(n, *arrays):
    s3, s4, s5, l3, l4, l5, lb3, lb4, lb5, o3, o4, o5, ob3, ob4, ob5 = arrays
    dims = tuple(x.shape[1:3] for x in (s3, s4, s5))
    fd = l3.shape[1]
    (rows3, wid3), (rows4, wid4), (rows5, wid5) = dims
    flat = [x.reshape(-1, x.shape[3]) for x in (s3, s4, s5)]
    biases = [b.reshape(1, fd) for b in (lb3, lb4, lb5, ob3, ob4, ob5)]
    anywhere, vmem = pl.BlockSpec(memory_space=pl.ANY), pl.BlockSpec(memory_space=pltpu.VMEM)
    far = max(n // 2, 1)

    def array(*shape):
        return pltpu.VMEM(shape, BF16)

    def result(pixels):
        return jax.ShapeDtypeStruct((pixels, fd), BF16)

    dma = pltpu.SemaphoreType.DMA
    y3, y4, y5, y6 = pl.pallas_call(
        functools.partial(kernel, n, dims),
        out_shape=(
            result(rows3 * wid3),
            result(rows4 * wid4),
            result(n * rows5 * wid5),
            result(n * rows5 * wid5 // 4),
        ),
        in_specs=[anywhere] * 6 + [vmem] * 3 + [anywhere] * 3 + [vmem] * 3,
        out_specs=(anywhere,) * 4,
        scratch_shapes=[
            *(array(*x.shape) for x in flat),
            array(n * l5.shape[0], fd),
            array(n * l4.shape[0], fd),
            array(n * l3.shape[0], fd),
            *(array(3, 3, n * x.shape[2], fd) for x in (o3, o5, o4)),
            array((rows3 + 2) * wid3, fd),
            array((rows4 + 2) * wid4, fd),
            array((n * rows5 + 2) * wid5, fd),
            array(rows3 * wid3, fd),
            array(rows4 * wid4, fd),
            array(n * rows5 * wid5, fd),
            array(n * rows5 * wid5 // 4, fd),
            dma((7, 2, far)),
            dma((7, 2, far)),
            dma((6, n - 1)),
            dma((6, n - 1)),
            dma((4,)),
            dma((4,)),
            dma((13,)),
        ],
        compiler_params=pltpu.CompilerParams(
            collective_id=0, has_side_effects=True, vmem_limit_bytes=48 * 1024 * 1024
        ),
    )(*flat, l3, l4, l5, *biases[:3], o3, o4, o5, *biases[3:])
    return (
        y3.reshape(1, rows3, wid3, fd),
        y4.reshape(1, rows4, wid4, fd),
        y5.reshape(1, n * rows5, wid5, fd),
        y6.reshape(1, n * rows5 // 2, wid5 // 2, fd),
    )


def solution(mesh):
    split, rows = P("dp", "space", None, None), P("space", None)
    taps = P(None, None, "space", None)
    whole = P("dp", None, None, None)
    return jax.shard_map(
        functools.partial(on_device, mesh.shape["space"]),
        mesh=mesh,
        in_specs=(split,) * 3 + (rows,) * 3 + (P(),) * 3 + (taps,) * 3 + (P(),) * 3,
        out_specs=(split, split, whole, whole),
        check_vma=False,
    )
```

```python
import functools

import jax
import jax.numpy as jnp
from jax import lax
from jax.experimental import pallas as pl
from jax.experimental.pallas import tpu as pltpu
from jax.sharding import PartitionSpec as P

F32, BF16 = jnp.float32, jnp.bfloat16


def ring_place(s, n):
    return s // 2 + (s % 2) * (n - 1 - 2 * (s // 2))


def ring_owner(place, n):
    r = (place + 2 * n) % n
    back = r // (n // 2)
    return (1 - back) * (2 * r) + back * (2 * (n - 1 - r) + 1)


def spread(coarse):
    pixels = coarse.shape[0]
    fine = lax.broadcasted_iota(jnp.int32, (2 * pixels, pixels), 0) // 2
    pick = (fine == lax.broadcasted_iota(jnp.int32, (2 * pixels, pixels), 1)).astype(BF16)
    return jnp.dot(pick, coarse, preferred_element_type=F32)


def conv_tile(frame, weight, bias, start, pixels, width):
    rows = jnp.concatenate(
        [frame[pl.ds(pl.multiple_of(start + a * width, 16), pixels), :] for a in range(3)], axis=1
    )
    depth = weight.shape[2]
    part = [
        jnp.dot(
            rows,
            weight[:, c].reshape(3 * depth, weight.shape[3]),
            preferred_element_type=F32,
        )
        for c in range(3)
    ]
    column = lax.broadcasted_iota(jnp.int32, (pixels, 1), 0) % width
    left = jnp.where(column == 0, 0.0, pltpu.roll(part[0], 1, 0))
    right = jnp.where(column == width - 1, 0.0, pltpu.roll(part[2], pixels - 1, 0))
    return part[1] + left + right + bias[...]


def kernel(
    n, dims,
    s3, s4, s5, l3, l4, l5, hb3, hb4, hb5, o3, o4, o5, hc3, hc4, hc5,
    y3, y4, y5, y6,
    v3, v4, v5, w_l5, w_l4, w_l3, w_o3, w_o5, w_o4,
    m3, m4, m5, r3, r4, r5, r6, lb3, lb4, lb5, ob3, ob4, ob5,
    ring_send, ring_recv, core_send, core_recv, map_send, map_recv, halo_send, halo_recv, local_sem,
):
    (rows3, wid3), (rows4, wid4), (rows5, wid5) = dims
    dp, s = lax.axis_index("dp"), lax.axis_index("space")
    core = dp % 2
    partner = (dp + 1 - 2 * core, s)
    place = ring_place(s, n)
    sign = 1 - 2 * core
    hops = (n // 2, n - 1 - n // 2)
    turn = (sign, -sign)
    target = [(dp, ring_owner(place + turn[k], n)) for k in range(2)]
    above, below = (dp, (s + n - 1) % n), (dp, (s + 1) % n)

    full = (w_l5, w_l4, w_l3, w_o3, w_o5, w_o4)
    mine = (l5, l4, l3, o3, o5, o4)
    half = w_l5.shape[1] // 2

    def map_rows(owner):
        size = rows5 * wid5
        return m5.at[pl.ds(pl.multiple_of(wid5 + owner * size, 16), size), :]

    def chunk(a, owner, side):
        cols = pl.ds(pl.multiple_of(side * half, half), half)
        if a < 3:
            size = mine[a].shape[0]
            return full[a].at[pl.ds(pl.multiple_of(owner * size, size), size), cols]
        size = mine[a].shape[2]
        return full[a].at[:, :, pl.ds(pl.multiple_of(owner * size, size), size), cols]

    def own_part(a):
        cols = pl.ds(pl.multiple_of(core * half, half), half)
        return mine[a].at[:, cols] if a < 3 else mine[a].at[:, :, :, cols]

    def own_whole(a):
        if a < 3:
            size = mine[a].shape[0]
            return full[a].at[pl.ds(pl.multiple_of(s * size, size), size), :]
        size = mine[a].shape[2]
        return full[a].at[:, :, pl.ds(pl.multiple_of(s * size, size), size), :]

    local = [pltpu.make_async_copy(mine[a], own_whole(a), local_sem.at[a]) for a in range(6)]
    features = [
        pltpu.make_async_copy(src, dst, local_sem.at[6 + k])
        for k, (src, dst) in enumerate(((s5, v5), (s4, v4), (s3, v3)))
    ]
    biases = [
        pltpu.make_async_copy(src, dst, local_sem.at[13 + k])
        for k, (src, dst) in enumerate(
            ((hb3, lb3), (hb4, lb4), (hb5, lb5), (hc3, ob3), (hc4, ob4), (hc5, ob5))
        )
    ]
    for copy in features + local + biases:
        copy.start()

    barrier = pltpu.get_barrier_semaphore()
    peers = [(dp, (s + d) % n) for d in range(1, n)]
    for device in (*peers, partner):
        pl.semaphore_signal(
            barrier, inc=1, device_id=device, device_id_type=pl.DeviceIdType.MESH
        )
    pl.semaphore_wait(barrier, n)

    def remote(src, dst, send, recv, device):
        return pltpu.make_async_remote_copy(
            src_ref=src, dst_ref=dst, send_sem=send, recv_sem=recv,
            device_id=device, device_id_type=pl.DeviceIdType.MESH,
        )

    sent = []

    def push(a, k, step):
        if step > hops[k]:
            return
        owner = ring_owner(place - turn[k] * (step - 1), n)
        dst = chunk(a, owner, core)
        src = own_part(a) if step == 1 else dst
        copy = remote(src, dst, ring_send.at[a, k, step - 1], ring_recv.at[a, k, step - 1], target[k])
        copy.start()
        sent.append(copy)

    def cross(a, k, step, side, turns):
        owner = ring_owner(place - turns[k] * step, n)
        spot = chunk(a, owner, side)
        j = k * hops[0] + step - 1
        return remote(spot, spot, core_send.at[a, j], core_recv.at[a, j], partner)

    def pull(a, step):
        for k in range(2):
            if step > hops[k]:
                continue
            owner = ring_owner(place - turn[k] * step, n)
            spot = chunk(a, owner, core)
            remote(
                spot, spot, ring_send.at[a, k, step - 1], ring_recv.at[a, k, step - 1], target[k]
            ).wait_recv()
            push(a, k, step + 1)
            copy = cross(a, k, step, core, turn)
            copy.start()
            sent.append(copy)

    def settle(a):
        for k in range(2):
            for step in range(1, hops[k] + 1):
                cross(a, k, step, 1 - core, (turn[1], turn[0])).wait_recv()
        local[a].wait()

    for a in (0, 1, 2):
        push(a, 0, 1)
        push(a, 1, 1)
    waiting = [3, 4, 5]
    for step in range(1, hops[0] + 1):
        if waiting and step > 1:
            a = waiting.pop(0)
            push(a, 0, 1)
            push(a, 1, 1)
        for a in (0, 1, 2):
            pull(a, step)
    while waiting:
        a = waiting.pop(0)
        push(a, 0, 1)
        push(a, 1, 1)
    for a in (3, 4, 5):
        pull(a, 1)

    settle(0)
    features[0].wait()
    for copy in biases:
        copy.wait()
    zero5 = jnp.zeros((wid5, m5.shape[1]), BF16)
    m5[pl.ds(0, wid5), :] = zero5
    m5[pl.ds(m5.shape[0] - wid5, wid5), :] = zero5
    here = pl.multiple_of(wid5 + s * (rows5 * wid5), 16)
    m5[pl.ds(here, rows5 * wid5), :] = (
        jnp.dot(v5[...], w_l5[...], preferred_element_type=F32) + lb5[...]
    ).astype(BF16)
    settle(1)
    features[1].wait()
    for d in range(1, n):
        copy = remote(map_rows(s), map_rows(s), map_send.at[d - 1], map_recv.at[d - 1], peers[d - 1])
        copy.start()
        sent.append(copy)
    for r in range(rows5):
        up = spread(m5[pl.ds(pl.multiple_of(here + r * wid5, 16), wid5), :])
        base = 2 * r * wid4
        lat = jnp.dot(v4[base : base + 2 * wid4, :], w_l4[...], preferred_element_type=F32)
        m4[wid4 + base : wid4 + base + 2 * wid4, :] = (
            lat + lb4[...] + jnp.concatenate([up, up], axis=0)
        ).astype(BF16)
    settle(2)
    features[2].wait()

    def coarse_row(r, carry):
        up = spread(m4[pl.ds(pl.multiple_of(wid4 + r * wid4, 16), wid4), :])
        base = pl.multiple_of(2 * r * wid3, 16)
        lat = jnp.dot(v3[pl.ds(base, 2 * wid3), :], w_l3[...], preferred_element_type=F32)
        m3[pl.ds(pl.multiple_of(wid3 + base, 16), 2 * wid3), :] = (
            lat + lb3[...] + jnp.concatenate([up, up], axis=0)
        ).astype(BF16)
        return carry

    lax.fori_loop(0, rows4 // 2, coarse_row, 0)
    for a in (3, 4, 5):
        pull(a, 2)
    lax.fori_loop(rows4 // 2, rows4, coarse_row, 0)

    halos = []
    for k, (frame, rows, wid) in enumerate(((m4, rows4, wid4), (m3, rows3, wid3))):
        first, last = frame.at[pl.ds(wid, wid), :], frame.at[pl.ds(rows * wid, wid), :]
        top, bottom = frame.at[pl.ds(0, wid), :], frame.at[pl.ds((rows + 1) * wid, wid), :]
        halos.append((
            remote(last, top, halo_send.at[2 * k], halo_recv.at[2 * k], below),
            remote(first, bottom, halo_send.at[2 * k + 1], halo_recv.at[2 * k + 1], above),
        ))

    def start_halos():
        @pl.when(s < n - 1)
        def _():
            for pair in halos:
                pair[0].start()

        @pl.when(s > 0)
        def _():
            for pair in halos:
                pair[1].start()

    for step in range(3, hops[0]):
        for a in (3, 4, 5):
            pull(a, step)
            if step == 3 and a == 3:
                start_halos()
    pull(3, hops[0])

    @pl.when(s > 0)
    def _():
        for pair in halos:
            pair[0].wait_recv()
            pair[1].wait_send()

    @pl.when(s < n - 1)
    def _():
        for pair in halos:
            pair[1].wait_recv()
            pair[0].wait_send()

    for frame, rows, wid in ((m4, rows4, wid4), (m3, rows3, wid3)):
        zero = jnp.zeros((wid, frame.shape[1]), BF16)

        @pl.when(s == 0)
        def _():
            frame[pl.ds(0, wid), :] = zero

        @pl.when(s == n - 1)
        def _():
            frame[pl.ds((rows + 1) * wid, wid), :] = zero

    settle(3)

    def conv(frame, weight, bias, out, rows, wid, tall):
        def tile(i, carry):
            start = pl.multiple_of(i * (tall * wid), 16)
            out[pl.ds(start, tall * wid), :] = conv_tile(
                frame, weight, bias, start, tall * wid, wid
            ).astype(BF16)
            return carry

        lax.fori_loop(0, rows // tall, tile, 0)

    conv(m3, w_o3, ob3, r3, rows3, wid3, 4)
    out3 = pltpu.make_async_copy(r3, y3, local_sem.at[9])
    out3.start()

    pull(4, hops[0])
    pull(5, hops[0])
    settle(4)
    for d in range(1, n):
        spot = map_rows((s + n - d) % n)
        remote(spot, spot, map_send.at[d - 1], map_recv.at[d - 1], peers[d - 1]).wait_recv()
    conv(m5, w_o5, ob5, r5, n * rows5, wid5, 16)
    out5 = pltpu.make_async_copy(r5, y5, local_sem.at[10])
    out5.start()
    take = lax.broadcasted_iota(jnp.int32, (wid5 // 2, wid5), 0) * 2
    pick = (take == lax.broadcasted_iota(jnp.int32, (wid5 // 2, wid5), 1)).astype(BF16)

    def even_row(i, carry):
        row = r5[pl.ds(pl.multiple_of(2 * i * wid5, 16), wid5), :]
        r6[pl.ds(pl.multiple_of(i * (wid5 // 2), 16), wid5 // 2), :] = jnp.dot(
            pick, row, preferred_element_type=F32
        ).astype(BF16)
        return carry

    lax.fori_loop(0, n * rows5 // 2, even_row, 0)
    out6 = pltpu.make_async_copy(r6, y6, local_sem.at[11])
    out6.start()

    settle(5)
    conv(m4, w_o4, ob4, r4, rows4, wid4, rows4)
    out4 = pltpu.make_async_copy(r4, y4, local_sem.at[12])
    out4.start()

    for copy in sent:
        copy.wait_send()
    for copy in (out3, out5, out6, out4):
        copy.wait()


def on_device(n, *arrays):
    s3, s4, s5, l3, l4, l5, lb3, lb4, lb5, o3, o4, o5, ob3, ob4, ob5 = arrays
    dims = tuple(x.shape[1:3] for x in (s3, s4, s5))
    fd = l3.shape[1]
    (rows3, wid3), (rows4, wid4), (rows5, wid5) = dims
    flat = [x.reshape(-1, x.shape[3]) for x in (s3, s4, s5)]
    biases = [b.reshape(1, fd) for b in (lb3, lb4, lb5, ob3, ob4, ob5)]
    anywhere = pl.BlockSpec(memory_space=pl.ANY)
    far = max(n // 2, 1)

    def array(*shape):
        return pltpu.VMEM(shape, BF16)

    def result(pixels):
        return jax.ShapeDtypeStruct((pixels, fd), BF16)

    dma = pltpu.SemaphoreType.DMA
    y3, y4, y5, y6 = pl.pallas_call(
        functools.partial(kernel, n, dims),
        out_shape=(
            result(rows3 * wid3),
            result(rows4 * wid4),
            result(n * rows5 * wid5),
            result(n * rows5 * wid5 // 4),
        ),
        in_specs=[anywhere] * 15,
        out_specs=(anywhere,) * 4,
        scratch_shapes=[
            *(array(*x.shape) for x in flat),
            array(n * l5.shape[0], fd),
            array(n * l4.shape[0], fd),
            array(n * l3.shape[0], fd),
            *(array(3, 3, n * x.shape[2], fd) for x in (o3, o5, o4)),
            array((rows3 + 2) * wid3, fd),
            array((rows4 + 2) * wid4, fd),
            array((n * rows5 + 2) * wid5, fd),
            array(rows3 * wid3, fd),
            array(rows4 * wid4, fd),
            array(n * rows5 * wid5, fd),
            array(n * rows5 * wid5 // 4, fd),
            *(pltpu.VMEM((1, fd), F32) for _ in range(6)),
            dma((6, 2, far)),
            dma((6, 2, far)),
            dma((6, n - 1)),
            dma((6, n - 1)),
            dma((n - 1,)),
            dma((n - 1,)),
            dma((4,)),
            dma((4,)),
            dma((19,)),
        ],
        compiler_params=pltpu.CompilerParams(
            collective_id=0, has_side_effects=True, vmem_limit_bytes=60 * 1024 * 1024
        ),
    )(*flat, l3, l4, l5, *biases[:3], o3, o4, o5, *biases[3:])
    return (
        y3.reshape(1, rows3, wid3, fd),
        y4.reshape(1, rows4, wid4, fd),
        y5.reshape(1, n * rows5, wid5, fd),
        y6.reshape(1, n * rows5 // 2, wid5 // 2, fd),
    )


def solution(mesh):
    split, rows = P("dp", "space", None, None), P("space", None)
    taps = P(None, None, "space", None)
    whole = P("dp", None, None, None)
    return jax.shard_map(
        functools.partial(on_device, mesh.shape["space"]),
        mesh=mesh,
        in_specs=(split,) * 3 + (rows,) * 3 + (P(),) * 3 + (taps,) * 3 + (P(),) * 3,
        out_specs=(split, split, whole, whole),
        check_vma=False,
    )
```
